32 devices in a mesh: grp: 16 (over z, y, core), seq: 2 (over x).
Axes of the slice: x: 2, y: 2, z: 4, core: 2. Of those that a mesh axis runs over, the one named last changes fastest.
Arguments:
- queries: bfloat16 [8192, 4096], P(('grp', 'seq')), may hold values from -8 to 8
- keys: bfloat16 [8192, 4096], P(('grp', 'seq')), may hold values from -6 to 6
- values: bfloat16 [8192, 4096], P(('grp', 'seq')), may hold values from -6 to 6
- global_pos: int32 [64], P(('grp', 'seq')), may hold values from 0 to 127
- layout: int32 [64, 32], P(('grp', 'seq')), may hold values from 0 to 63, all different within a row
Outputs:
- attended: bfloat16 [8192, 4096], P(('grp', 'seq'))
The draws below stay inside these ranges and needn't reach their ends.
Inputs may be any that keep to these rules, and one draw needn't show every extreme that they name: `layout`: each row lists 32 different block indices, and every block is listed by some row.
All inputs are finite; a program needn't handle non-finite values.
Results may differ from the reference program's by a relative error of at most 0.0042.
Values may be sent and summed in bfloat16 or wider, within the bound.
A program may use at most 128 MiB of HBM per device.

```python
import math
import jax
import jax.numpy as jnp
from jax import lax

HEADS = 32
HEAD_DIM = 128
BLOCK = 128
LINKS = 32
WIDTH = 4096
SEQ = 8192
NBLK = 64


def draw_queries(key, part):
    base = jnp.clip(2.0 * jax.random.normal(jax.random.fold_in(key, 1), (SEQ, HEADS * HEAD_DIM), jnp.float32), -8.0, 8.0)
    return base.astype(jnp.bfloat16)


def draw_keys(key, part):
    base = jnp.clip(jax.random.normal(jax.random.fold_in(key, 2), (SEQ, HEADS * HEAD_DIM), jnp.float32), -6.0, 6.0)
    return base.astype(jnp.bfloat16)


def with_ends(entries, key, smallest, largest):
    longest = entries.shape.index(max(entries.shape))
    spots = []
    for shift in (0, 1):
        where = [jax.random.randint(jax.random.fold_in(key, axis), (), 0, length) for axis, length in enumerate(entries.shape)]
        where[longest] = (where[longest] + shift) % entries.shape[longest]
        spots.append(tuple(where))
    return entries.at[spots[0]].set(smallest).at[spots[1]].set(largest)


def shard_levels(key, extent, pieces, smallest, high):
    def one(dim, shards_of):
        heights = jax.random.uniform(jax.random.fold_in(jax.random.fold_in(key, 6), dim), (shards_of,), jnp.float32, smallest / len(pieces), high / len(pieces))
        return jnp.repeat(jnp.exp(heights), extent[dim] // shards_of).reshape((-1,) + (1,) * (len(extent) - dim - 1))

    factor_of = one(*pieces[0])
    for cut in pieces[1:]:
        factor_of = factor_of * one(*cut)
    return factor_of


def picks_of(key, rows, amount, top, lift):
    sequence = jax.random.permutation(jax.random.fold_in(key, 1), amount)
    boost = sequence
    for power in range(3):
        boost = boost * boost // amount
    boost = boost * lift // amount
    lots = jax.random.randint(jax.random.fold_in(key, 2), (rows, amount), 0, 4096) + boost
    sure = jax.random.permutation(jax.random.fold_in(key, 3), rows)[jnp.arange(amount) % rows]
    lots = jnp.where(jnp.arange(rows)[:, None] == sure[None, :], 1 << 14, lots)
    merit = lots * amount + jnp.arange(amount)
    return lax.top_k(merit.astype(jnp.int32), top)[1].astype(jnp.int32)


def noise(rng, dims, scale, reach, split=(), kind=jnp.bfloat16):
    values = jax.random.normal(rng, dims, jnp.float32) * scale
    if len(split) > 0:
        values = shard_levels(rng, dims, split, -0.22, 0.18) * values
    return jnp.clip(values, min=-reach, max=reach).astype(kind)


def setup_inputs(seed: int = 0) -> dict:
    seeds = jax.random.split(jax.random.key(seed), 6)
    return {
        "queries": draw_queries(jax.random.fold_in(seeds[5], 71), 0),
        "keys": draw_keys(jax.random.fold_in(seeds[5], 71), 0),
        "values": noise(seeds[2], (SEQ, WIDTH), 1.0, 6.0, ((0, 32),)),
        "global_pos": with_ends(jax.random.randint(seeds[3], (NBLK,), 0, BLOCK), jax.random.fold_in(seeds[3], 1), 0, BLOCK - 1).astype(jnp.int32),
        "layout": picks_of(seeds[4], NBLK, NBLK, LINKS, 0),
    }


def pooled(source, blocks_all):
    blocks = source.astype(jnp.float32).reshape(blocks_all, BLOCK, HEADS, HEAD_DIM).mean(axis=1)
    spread = lax.optimization_barrier(jnp.mean(blocks * blocks, axis=-1, keepdims=True))
    return (blocks / jnp.sqrt(spread + 1e-06)).reshape(blocks_all, HEADS * HEAD_DIM).astype(jnp.bfloat16)

def reference(queries, keys, values, global_pos, layout):
    score_scale = 1.0 / math.sqrt(HEAD_DIM)
    summary_keys = pooled(keys, NBLK).astype(jnp.float32).reshape(NBLK, HEADS, HEAD_DIM)
    summary_values = pooled(values, NBLK).astype(jnp.float32).reshape(NBLK, HEADS, HEAD_DIM)
    padding = jnp.zeros((BLOCK, HEADS * HEAD_DIM), jnp.bfloat16)
    padded_keys = jnp.concatenate([padding, keys, padding], axis=0)
    padded_values = jnp.concatenate([padding, values, padding], axis=0)
    block_ids = jnp.arange(NBLK, dtype=jnp.int32)

    def one_block(which):
        first_row = (which * BLOCK).astype(jnp.int32)
        query_rows = lax.dynamic_slice_in_dim(queries, first_row, BLOCK, 0).astype(jnp.float32).reshape(BLOCK, HEADS, HEAD_DIM)
        window_keys = lax.dynamic_slice_in_dim(padded_keys, first_row, 3 * BLOCK, 0).astype(jnp.float32).reshape(3 * BLOCK, HEADS, HEAD_DIM)
        window_values = lax.dynamic_slice_in_dim(padded_values, first_row, 3 * BLOCK, 0).astype(jnp.float32).reshape(3 * BLOCK, HEADS, HEAD_DIM)
        window_scores = jnp.einsum('qhd,khd->hqk', query_rows, window_keys) * score_scale
        key_block = jnp.arange(3 * BLOCK, dtype=jnp.int32) // BLOCK + which - 1
        inside = (key_block >= 0) & (key_block < NBLK)
        window_scores = jnp.where(inside[None, None, :], window_scores, -jnp.inf)
        summary_scores = jnp.einsum('qhd,jhd->hqj', query_rows, summary_keys) * score_scale
        listed = jnp.any(layout[which][:, None] == block_ids[None, :], axis=0)
        is_global = jnp.arange(BLOCK, dtype=jnp.int32) == global_pos[which]
        visible = listed[None, :] | is_global[:, None]
        summary_scores = jnp.where(visible[None, :, :], summary_scores, -jnp.inf)
        peak = jnp.maximum(lax.optimization_barrier(jnp.max(window_scores, axis=-1)), lax.optimization_barrier(jnp.max(summary_scores, axis=-1)))
        window_weights = jnp.exp(window_scores - peak[..., None])
        summary_weights = jnp.exp(summary_scores - peak[..., None])
        denominator = lax.optimization_barrier(jnp.sum(window_weights, axis=-1)) + lax.optimization_barrier(jnp.sum(summary_weights, axis=-1))
        rounded_window = lax.optimization_barrier(window_weights.astype(jnp.bfloat16)).astype(jnp.float32)
        rounded_summary = lax.optimization_barrier(summary_weights.astype(jnp.bfloat16)).astype(jnp.float32)
        numerator = jnp.einsum('hqk,khd->hqd', rounded_window, window_values)
        numerator = numerator + jnp.einsum('hqj,jhd->hqd', rounded_summary, summary_values)
        result = numerator / denominator[..., None]
        return jnp.transpose(result, (1, 0, 2)).reshape(BLOCK, HEADS * HEAD_DIM).astype(jnp.bfloat16)
    outputs = lax.map(one_block, block_ids)
    return outputs.reshape(SEQ, HEADS * HEAD_DIM)
```

```python
import functools
import math

import jax
import jax.numpy as jnp
from jax import lax
from jax.experimental import pallas as pl
from jax.experimental.pallas import tpu as pltpu
from jax.sharding import PartitionSpec as P

HEAD_DIM = 128
BLOCK = 128
CHUNK_HEADS = 2
POOL_HEADS = 8
MESH = pl.DeviceIdType.MESH


def dot_t(a, b):
    return lax.dot_general(a, b, (((1,), (1,)), ((), ())), preferred_element_type=jnp.float32)


def dot(a, b):
    return jnp.dot(a, b, preferred_element_type=jnp.float32)


def kernel(
    groups, seqs, pos_ref, layout_ref, q_hbm, k_hbm, v_hbm, out_hbm,
    q, k, v, out, halo, gathered, own, wide, bias,
    load_sem, store_sem, send_sem, recv_sem, seq_send, seq_recv, grp_send, grp_recv,
):
    rows, width = q.shape
    heads = width // HEAD_DIM
    blocks = rows // BLOCK
    devices = groups * seqs
    total_blocks = devices * blocks
    step_cols = CHUNK_HEADS * HEAD_DIM
    chunks = heads // CHUNK_HEADS
    stages = groups.bit_length() - 1
    near = 2 * seqs

    g, s = lax.axis_index("grp"), lax.axis_index("seq")
    me = g * seqs + s
    has_left, has_right = me > 0, me < devices - 1
    left, right = lax.max(me - 1, 0), lax.min(me + 1, devices - 1)

    def coords(position):
        return (position // seqs, position % seqs)

    left_near = has_left & (me % near != 0)
    right_near = has_right & ((me + 1) % near != 0)
    left_far = has_left & (me % near == 0)
    right_far = has_right & ((me + 1) % near == 0)

    loads = [
        pltpu.make_async_copy(src, dst, load_sem.at[i])
        for i, (src, dst) in enumerate(((k_hbm, k), (v_hbm, v), (q_hbm, q)))
    ]
    for load in loads:
        load.start()

    barrier = pltpu.get_barrier_semaphore()

    def signal(device):
        pl.semaphore_signal(barrier, inc=1, device_id=device, device_id_type=MESH)

    @pl.when(has_left)
    def _():
        signal(coords(left))

    @pl.when(has_right)
    def _():
        signal(coords(right))

    for o in range(1, seqs):
        signal((g, lax.rem(s + o, seqs)))

    def partner(stage):
        size = 1 << stage
        bit = (g // size) % 2
        return g + size * (1 - 2 * bit)

    for stage in range(stages):
        signal((partner(stage), s))
    pl.semaphore_wait(
        barrier, seqs - 1 + stages + has_left.astype(jnp.int32) + has_right.astype(jnp.int32)
    )

    def edge(side, kv, c):
        src = (k_hbm, v_hbm)[kv]
        cols = pl.ds(pl.multiple_of(c * step_cols, step_cols), step_cols)
        first = rows - BLOCK if side == 0 else 0
        return pltpu.make_async_remote_copy(
            src_ref=src.at[pl.ds(first, BLOCK), cols],
            dst_ref=halo.at[side, kv, :, cols],
            send_sem=send_sem.at[side, kv, c],
            recv_sem=recv_sem.at[side, kv, c],
            device_id=coords(right if side == 0 else left),
            device_id_type=MESH,
        )

    def send_edges(side, when, lo, hi):
        @pl.when(when)
        def _():
            def body(c, carry):
                for kv in range(2):
                    edge(side, kv, c).start()
                return carry

            lax.fori_loop(lo, hi, body, 0)

    def send_both(when_right, when_left, lo, hi):
        both = when_right & when_left

        @pl.when(both)
        def _():
            def body(c, carry):
                for side in range(2):
                    for kv in range(2):
                        edge(side, kv, c).start()
                return carry

            lax.fori_loop(lo, hi, body, 0)

        send_edges(0, when_right & jnp.logical_not(when_left), lo, hi)
        send_edges(1, when_left & jnp.logical_not(when_right), lo, hi)

    send_both(right_near, left_near, 0, 1)

    loads[0].wait()
    loads[1].wait()
    picks = (
        lax.broadcasted_iota(jnp.int32, (16, rows), 1) // BLOCK
        == lax.broadcasted_iota(jnp.int32, (16, rows), 0)
    ).astype(jnp.bfloat16)

    def pool(step, carry):
        for i in range(POOL_HEADS):
            h = step * POOL_HEADS + i
            cols = pl.ds(pl.multiple_of(h * HEAD_DIM, HEAD_DIM), HEAD_DIM)
            for kv, src in enumerate((k, v)):
                mean = dot(picks, src[:, cols])[:8] * (1.0 / BLOCK)
                spread = jnp.mean(mean * mean, axis=-1, keepdims=True)
                scaled = mean / jnp.sqrt(spread + 1e-06)
                for b in range(blocks):
                    own[pl.ds((kv * blocks + b) * heads + h, 1), :] = scaled[b : b + 1]
        return carry

    lax.fori_loop(0, heads // POOL_HEADS, pool, 0)
    gathered[me] = own[...].astype(jnp.bfloat16)

    def seq_copy(o):
        return pltpu.make_async_remote_copy(
            src_ref=gathered.at[pl.ds(me, 1)],
            dst_ref=gathered.at[pl.ds(me, 1)],
            send_sem=seq_send.at[o],
            recv_sem=seq_recv.at[o],
            device_id=(g, lax.rem(s + o, seqs)),
            device_id_type=MESH,
        )

    for o in range(1, seqs):
        seq_copy(o).start()

    send_both(right_near, left_near, 1, chunks)

    ids = lax.broadcasted_iota(jnp.int32, (BLOCK, total_blocks), 1)
    spots = lax.broadcasted_iota(jnp.int32, (BLOCK, total_blocks), 0)
    for b in range(blocks):
        seen = spots == pos_ref[b]
        for link in range(layout_ref.shape[1]):
            seen = seen | (ids == layout_ref[b, link])
        bias[b * BLOCK : (b + 1) * BLOCK, :] = jnp.where(seen, 0.0, -jnp.inf)

    @pl.when(jnp.logical_not(has_left))
    def _():
        halo[0] = jnp.zeros(halo.shape[1:], halo.dtype)

    @pl.when(jnp.logical_not(has_right))
    def _():
        halo[1] = jnp.zeros(halo.shape[1:], halo.dtype)

    for o in range(1, seqs):
        seq_copy(o).wait()

    def grp_copy(stage):
        size = (1 << stage) * seqs
        first = (g // (1 << stage)) * size
        return pltpu.make_async_remote_copy(
            src_ref=gathered.at[pl.ds(first, size)],
            dst_ref=gathered.at[pl.ds(first, size)],
            send_sem=grp_send.at[stage],
            recv_sem=grp_recv.at[stage],
            device_id=(partner(stage), s),
            device_id_type=MESH,
        )

    for stage in range(stages):
        grp_copy(stage).start()
        if stage == stages - 1:
            send_both(right_far, left_far, 0, chunks)
        grp_copy(stage).wait()

    def widen(d, carry):
        spread = blocks * heads
        at = pl.ds(pl.multiple_of(d * spread, spread), spread)
        for kv in range(2):
            wide[kv, at, :] = gathered[d, kv * spread : (kv + 1) * spread].astype(jnp.float32)
        return carry

    lax.fori_loop(0, devices, widen, 0)
    loads[2].wait()

    factor = math.log2(math.e) / math.sqrt(HEAD_DIM)
    left_bias = jnp.where(has_left, 0.0, -jnp.inf)
    right_bias = jnp.where(has_right, 0.0, -jnp.inf)

    def store(c):
        cols = pl.ds(pl.multiple_of(c * step_cols, step_cols), step_cols)
        return pltpu.make_async_copy(out.at[:, cols], out_hbm.at[:, cols], store_sem.at[c])

    def attend(c, carry):
        for side, there in ((0, has_left), (1, has_right)):
            @pl.when(there)
            def _(side=side):
                for kv in range(2):
                    edge(side, kv, c).wait_recv()

        for i in range(CHUNK_HEADS):
            h = c * CHUNK_HEADS + i
            cols = pl.ds(pl.multiple_of(h * HEAD_DIM, HEAD_DIM), HEAD_DIM)
            rows_of = pl.ds(h, total_blocks, stride=heads)
            qh, kh, vh = q[:, cols], k[:, cols], v[:, cols]
            sk = wide[0, rows_of, :].astype(jnp.bfloat16)
            sv = wide[1, rows_of, :].astype(jnp.bfloat16)
            kl, vl = halo[0, 0, :, cols], halo[0, 1, :, cols]
            kr, vr = halo[1, 0, :, cols], halo[1, 1, :, cols]
            s_own = dot_t(qh, kh)
            if blocks > 2:
                gap = (
                    lax.broadcasted_iota(jnp.int32, (rows, rows), 0) // BLOCK
                    - lax.broadcasted_iota(jnp.int32, (rows, rows), 1) // BLOCK
                )
                s_own = jnp.where(jnp.abs(gap) <= 1, s_own, -jnp.inf)
            s_left = dot_t(qh[:BLOCK], kl) + left_bias
            s_right = dot_t(qh[rows - BLOCK :], kr) + right_bias
            s_sum = dot_t(qh, sk) + bias[...]
            middle = [jnp.full((rows - 2 * BLOCK, BLOCK), -jnp.inf)] if blocks > 2 else []
            s_halo = jnp.concatenate([s_left, *middle, s_right], axis=0)
            peak = jnp.maximum(
                jnp.max(s_sum, axis=-1, keepdims=True),
                jnp.maximum(
                    jnp.max(s_own, axis=-1, keepdims=True),
                    jnp.max(s_halo, axis=-1, keepdims=True),
                ),
            )
            w_own = jnp.exp2((s_own - peak) * factor)
            w_halo = jnp.exp2((s_halo - peak) * factor)
            w_sum = jnp.exp2((s_sum - peak) * factor)
            total = (
                jnp.sum(w_own, axis=-1, keepdims=True)
                + jnp.sum(w_halo, axis=-1, keepdims=True)
                + jnp.sum(w_sum, axis=-1, keepdims=True)
            )
            r_halo = w_halo.astype(jnp.bfloat16)
            acc = dot(w_own.astype(jnp.bfloat16), vh) + dot(w_sum.astype(jnp.bfloat16), sv)
            middle = [jnp.zeros((rows - 2 * BLOCK, HEAD_DIM), jnp.float32)] if blocks > 2 else []
            acc = acc + jnp.concatenate(
                [dot(r_halo[:BLOCK], vl), *middle, dot(r_halo[rows - BLOCK :], vr)], axis=0
            )
            out[:, cols] = (acc / total).astype(jnp.bfloat16)
        store(c).start()
        return carry

    lax.fori_loop(0, chunks, attend, 0)

    def finish(c, carry):
        store(c).wait()
        for side, there in ((0, has_right), (1, has_left)):
            @pl.when(there)
            def _(side=side):
                for kv in range(2):
                    edge(side, kv, c).wait_send()
        return carry

    lax.fori_loop(0, chunks, finish, 0)


def solution(mesh):
    groups, seqs = mesh.shape["grp"], mesh.shape["seq"]
    assert groups & (groups - 1) == 0

    def shards(queries, keys, values, global_pos, layout):
        rows, width = queries.shape
        blocks, heads = rows // BLOCK, width // HEAD_DIM
        devices = groups * seqs
        chunks = heads // CHUNK_HEADS
        stages = groups.bit_length() - 1
        return pl.pallas_call(
            functools.partial(kernel, groups, seqs),
            out_shape=jax.ShapeDtypeStruct((rows, width), jnp.bfloat16),
            in_specs=[pl.BlockSpec(memory_space=pltpu.SMEM)] * 2
            + [pl.BlockSpec(memory_space=pl.ANY)] * 3,
            out_specs=pl.BlockSpec(memory_space=pl.ANY),
            scratch_shapes=[
                pltpu.VMEM((rows, width), jnp.bfloat16),
                pltpu.VMEM((rows, width), jnp.bfloat16),
                pltpu.VMEM((rows, width), jnp.bfloat16),
                pltpu.VMEM((rows, width), jnp.bfloat16),
                pltpu.VMEM((2, 2, BLOCK, width), jnp.bfloat16),
                pltpu.VMEM((devices, 2 * blocks * heads, HEAD_DIM), jnp.bfloat16),
                pltpu.VMEM((2 * blocks * heads, HEAD_DIM), jnp.float32),
                pltpu.VMEM((2, devices * blocks * heads, HEAD_DIM), jnp.float32),
                pltpu.VMEM((rows, devices * blocks), jnp.float32),
                pltpu.SemaphoreType.DMA((3,)),
                pltpu.SemaphoreType.DMA((chunks,)),
                pltpu.SemaphoreType.DMA((2, 2, chunks)),
                pltpu.SemaphoreType.DMA((2, 2, chunks)),
                pltpu.SemaphoreType.DMA((seqs,)),
                pltpu.SemaphoreType.DMA((seqs,)),
                pltpu.SemaphoreType.DMA((max(stages, 1),)),
                pltpu.SemaphoreType.DMA((max(stages, 1),)),
            ],
            compiler_params=pltpu.CompilerParams(
                collective_id=0, has_side_effects=True, vmem_limit_bytes=60 * 1024 * 1024
            ),
        )(global_pos, layout, queries, keys, values)

    both = ("grp", "seq")
    in_specs = (P(both, None), P(both, None), P(both, None), P(both), P(both, None))
    return jax.shard_map(
        shards, mesh=mesh, in_specs=in_specs, out_specs=P(both, None), check_vma=False
    )
```

```python
import functools
import math

import jax
import jax.numpy as jnp
from jax import lax
from jax.experimental import pallas as pl
from jax.experimental.pallas import tpu as pltpu
from jax.sharding import PartitionSpec as P

HEAD_DIM = 128
BLOCK = 128
CHUNK_HEADS = 2
EARLY_CHUNKS = 4
POOL_HEADS = 8
MESH = pl.DeviceIdType.MESH


def dot_t(a, b):
    return lax.dot_general(a, b, (((1,), (1,)), ((), ())), preferred_element_type=jnp.float32)


def dot(a, b):
    return jnp.dot(a, b, preferred_element_type=jnp.float32)


def kernel(
    groups, seqs, pos_hbm, layout_hbm, q_hbm, k_hbm, v_hbm, out,
    pos_ref, layout_ref, q, k, v, halo, gathered, own, wide, bias,
    load_sem, send_sem, recv_sem, seq_send, seq_recv, grp_send, grp_recv,
):
    rows, width = q.shape
    heads = width // HEAD_DIM
    blocks = rows // BLOCK
    devices = groups * seqs
    total_blocks = devices * blocks
    step_cols = CHUNK_HEADS * HEAD_DIM
    chunks = heads // CHUNK_HEADS
    stages = groups.bit_length() - 1
    near = 2 * seqs

    g, s = lax.axis_index("grp"), lax.axis_index("seq")
    me = g * seqs + s
    has_left, has_right = me > 0, me < devices - 1
    left, right = lax.max(me - 1, 0), lax.min(me + 1, devices - 1)

    def coords(position):
        return (position // seqs, position % seqs)

    left_near = has_left & (me % near != 0)
    right_near = has_right & ((me + 1) % near != 0)
    left_far = has_left & (me % near == 0)
    right_far = has_right & ((me + 1) % near == 0)

    loads = [
        pltpu.make_async_copy(src, dst, load_sem.at[i])
        for i, (src, dst) in enumerate(((k_hbm, k), (v_hbm, v), (q_hbm, q), (pos_hbm, pos_ref), (layout_hbm, layout_ref)))
    ]
    for load in loads:
        load.start()

    barrier = pltpu.get_barrier_semaphore()

    def signal(device):
        pl.semaphore_signal(barrier, inc=1, device_id=device, device_id_type=MESH)

    @pl.when(has_left)
    def _():
        signal(coords(left))

    @pl.when(has_right)
    def _():
        signal(coords(right))

    for o in range(1, seqs):
        signal((g, lax.rem(s + o, seqs)))

    def partner(stage):
        size = 1 << stage
        bit = (g // size) % 2
        return g + size * (1 - 2 * bit)

    for stage in range(stages):
        signal((partner(stage), s))
    pl.semaphore_wait(
        barrier, seqs - 1 + stages + has_left.astype(jnp.int32) + has_right.astype(jnp.int32)
    )

    def edge(side, kv, c):
        src = (k_hbm, v_hbm)[kv]
        cols = pl.ds(pl.multiple_of(c * step_cols, step_cols), step_cols)
        first = rows - BLOCK if side == 0 else 0
        return pltpu.make_async_remote_copy(
            src_ref=src.at[pl.ds(first, BLOCK), cols],
            dst_ref=halo.at[side, kv, :, cols],
            send_sem=send_sem.at[side, kv, c],
            recv_sem=recv_sem.at[side, kv, c],
            device_id=coords(right if side == 0 else left),
            device_id_type=MESH,
        )

    def send_edges(side, when, lo, hi):
        @pl.when(when)
        def _():
            def body(c, carry):
                for kv in range(2):
                    edge(side, kv, c).start()
                return carry

            lax.fori_loop(lo, hi, body, 0)

    def send_both(when_right, when_left, lo, hi):
        both = when_right & when_left

        @pl.when(both)
        def _():
            def body(c, carry):
                for side in range(2):
                    for kv in range(2):
                        edge(side, kv, c).start()
                return carry

            lax.fori_loop(lo, hi, body, 0)

        send_edges(0, when_right & jnp.logical_not(when_left), lo, hi)
        send_edges(1, when_left & jnp.logical_not(when_right), lo, hi)

    early = min(EARLY_CHUNKS, chunks)
    later = (early + chunks) // 2
    send_both(right_near, left_near, 0, early)
    send_both(right_far, left_far, 0, early)

    loads[0].wait()
    loads[1].wait()
    picks = (
        lax.broadcasted_iota(jnp.int32, (16, rows), 1) // BLOCK
        == lax.broadcasted_iota(jnp.int32, (16, rows), 0)
    ).astype(jnp.bfloat16)

    def pool(step, carry):
        for i in range(POOL_HEADS):
            h = step * POOL_HEADS + i
            cols = pl.ds(pl.multiple_of(h * HEAD_DIM, HEAD_DIM), HEAD_DIM)
            for kv, src in enumerate((k, v)):
                mean = dot(picks, src[:, cols])[:8] * (1.0 / BLOCK)
                spread = jnp.mean(mean * mean, axis=-1, keepdims=True)
                scaled = mean / jnp.sqrt(spread + 1e-06)
                for b in range(blocks):
                    own[pl.ds((kv * blocks + b) * heads + h, 1), :] = scaled[b : b + 1]
        return carry

    lax.fori_loop(0, heads // POOL_HEADS, pool, 0)
    gathered[me] = own[...].astype(jnp.bfloat16)

    def seq_copy(o):
        return pltpu.make_async_remote_copy(
            src_ref=gathered.at[pl.ds(me, 1)],
            dst_ref=gathered.at[pl.ds(me, 1)],
            send_sem=seq_send.at[o],
            recv_sem=seq_recv.at[o],
            device_id=(g, lax.rem(s + o, seqs)),
            device_id_type=MESH,
        )

    for o in range(1, seqs):
        seq_copy(o).start()

    send_both(right_near, left_near, early, chunks)

    loads[3].wait()
    loads[4].wait()
    ids = lax.broadcasted_iota(jnp.int32, (BLOCK, total_blocks), 1)
    spots = lax.broadcasted_iota(jnp.int32, (BLOCK, total_blocks), 0)
    for b in range(blocks):
        seen = spots == pos_ref[b]
        for link in range(layout_ref.shape[1]):
            seen = seen | (ids == layout_ref[b, link])
        bias[b * BLOCK : (b + 1) * BLOCK, :] = jnp.where(seen, 0.0, -jnp.inf)

    @pl.when(jnp.logical_not(has_left))
    def _():
        halo[0] = jnp.zeros(halo.shape[1:], halo.dtype)

    @pl.when(jnp.logical_not(has_right))
    def _():
        halo[1] = jnp.zeros(halo.shape[1:], halo.dtype)

    for o in range(1, seqs):
        seq_copy(o).wait()

    def grp_copy(stage):
        size = (1 << stage) * seqs
        first = (g // (1 << stage)) * size
        return pltpu.make_async_remote_copy(
            src_ref=gathered.at[pl.ds(first, size)],
            dst_ref=gathered.at[pl.ds(first, size)],
            send_sem=grp_send.at[stage],
            recv_sem=grp_recv.at[stage],
            device_id=(partner(stage), s),
            device_id_type=MESH,
        )

    for stage in range(stages):
        grp_copy(stage).start()
        if stage == stages - 2:
            send_both(right_far, left_far, early, later)
        if stage == stages - 1:
            send_both(right_far, left_far, later if stages > 1 else early, chunks)
        grp_copy(stage).wait()

    def widen(d, carry):
        spread = blocks * heads
        at = pl.ds(pl.multiple_of(d * spread, spread), spread)
        for kv in range(2):
            wide[kv, at, :] = gathered[d, kv * spread : (kv + 1) * spread].astype(jnp.float32)
        return carry

    lax.fori_loop(0, devices, widen, 0)
    loads[2].wait()

    factor = math.log2(math.e) / math.sqrt(HEAD_DIM)
    left_bias = jnp.where(has_left, 0.0, -jnp.inf)
    right_bias = jnp.where(has_right, 0.0, -jnp.inf)

    def attend(c, carry):
        for side, there in ((0, has_left), (1, has_right)):
            @pl.when(there)
            def _(side=side):
                for kv in range(2):
                    edge(side, kv, c).wait_recv()

        for i in range(CHUNK_HEADS):
            h = c * CHUNK_HEADS + i
            cols = pl.ds(pl.multiple_of(h * HEAD_DIM, HEAD_DIM), HEAD_DIM)
            rows_of = pl.ds(h, total_blocks, stride=heads)
            qh, kh, vh = q[:, cols], k[:, cols], v[:, cols]
            sk = wide[0, rows_of, :].astype(jnp.bfloat16)
            sv = wide[1, rows_of, :].astype(jnp.bfloat16)
            kl, vl = halo[0, 0, :, cols], halo[0, 1, :, cols]
            kr, vr = halo[1, 0, :, cols], halo[1, 1, :, cols]
            s_own = dot_t(qh, kh)
            if blocks > 2:
                gap = (
                    lax.broadcasted_iota(jnp.int32, (rows, rows), 0) // BLOCK
                    - lax.broadcasted_iota(jnp.int32, (rows, rows), 1) // BLOCK
                )
                s_own = jnp.where(jnp.abs(gap) <= 1, s_own, -jnp.inf)
            s_left = dot_t(qh[:BLOCK], kl) + left_bias
            s_right = dot_t(qh[rows - BLOCK :], kr) + right_bias
            s_sum = dot_t(qh, sk) + bias[...]
            middle = [jnp.full((rows - 2 * BLOCK, BLOCK), -jnp.inf)] if blocks > 2 else []
            s_halo = jnp.concatenate([s_left, *middle, s_right], axis=0)
            peak = jnp.maximum(
                jnp.max(s_sum, axis=-1, keepdims=True),
                jnp.maximum(
                    jnp.max(s_own, axis=-1, keepdims=True),
                    jnp.max(s_halo, axis=-1, keepdims=True),
                ),
            )
            w_own = jnp.exp2((s_own - peak) * factor)
            w_halo = jnp.exp2((s_halo - peak) * factor)
            w_sum = jnp.exp2((s_sum - peak) * factor)
            total = (
                jnp.sum(w_own, axis=-1, keepdims=True)
                + jnp.sum(w_halo, axis=-1, keepdims=True)
                + jnp.sum(w_sum, axis=-1, keepdims=True)
            )
            r_halo = w_halo.astype(jnp.bfloat16)
            acc = dot(w_own.astype(jnp.bfloat16), vh) + dot(w_sum.astype(jnp.bfloat16), sv)
            middle = [jnp.zeros((rows - 2 * BLOCK, HEAD_DIM), jnp.float32)] if blocks > 2 else []
            acc = acc + jnp.concatenate(
                [dot(r_halo[:BLOCK], vl), *middle, dot(r_halo[rows - BLOCK :], vr)], axis=0
            )
            out[:, cols] = (acc / total).astype(jnp.bfloat16)
        return carry

    lax.fori_loop(0, chunks, attend, 0)

    def finish(c, carry):
        for side, there in ((0, has_right), (1, has_left)):
            @pl.when(there)
            def _(side=side):
                for kv in range(2):
                    edge(side, kv, c).wait_send()
        return carry

    lax.fori_loop(0, chunks, finish, 0)


def solution(mesh):
    groups, seqs = mesh.shape["grp"], mesh.shape["seq"]
    assert groups & (groups - 1) == 0

    def shards(queries, keys, values, global_pos, layout):
        rows, width = queries.shape
        blocks, heads = rows // BLOCK, width // HEAD_DIM
        devices = groups * seqs
        chunks = heads // CHUNK_HEADS
        stages = groups.bit_length() - 1
        summaries = devices * blocks * width
        limit = 2 * (4 * rows + 4 * BLOCK) * width + 12 * summaries + (8 << 20)
        operands = [
            pltpu.with_memory_space_constraint(a, pltpu.HBM)
            for a in (global_pos, layout, queries, keys, values)
        ]
        return pl.pallas_call(
            functools.partial(kernel, groups, seqs),
            out_shape=pltpu.VMEM((rows, width), jnp.bfloat16),
            in_specs=[pl.BlockSpec(memory_space=pltpu.HBM)] * 5,
            out_specs=pl.BlockSpec(memory_space=pltpu.VMEM),
            scratch_shapes=[
                pltpu.SMEM(global_pos.shape, jnp.int32),
                pltpu.SMEM(layout.shape, jnp.int32),
                pltpu.VMEM((rows, width), jnp.bfloat16),
                pltpu.VMEM((rows, width), jnp.bfloat16),
                pltpu.VMEM((rows, width), jnp.bfloat16),
                pltpu.VMEM((2, 2, BLOCK, width), jnp.bfloat16),
                pltpu.VMEM((devices, 2 * blocks * heads, HEAD_DIM), jnp.bfloat16),
                pltpu.VMEM((2 * blocks * heads, HEAD_DIM), jnp.float32),
                pltpu.VMEM((2, devices * blocks * heads, HEAD_DIM), jnp.float32),
                pltpu.VMEM((rows, devices * blocks), jnp.float32),
                pltpu.SemaphoreType.DMA((5,)),
                pltpu.SemaphoreType.DMA((2, 2, chunks)),
                pltpu.SemaphoreType.DMA((2, 2, chunks)),
                pltpu.SemaphoreType.DMA((seqs,)),
                pltpu.SemaphoreType.DMA((seqs,)),
                pltpu.SemaphoreType.DMA((max(stages, 1),)),
                pltpu.SemaphoreType.DMA((max(stages, 1),)),
            ],
            compiler_params=pltpu.CompilerParams(
                collective_id=0, has_side_effects=True, vmem_limit_bytes=limit
            ),
        )(*operands)

    both = ("grp", "seq")
    in_specs = (P(both, None), P(both, None), P(both, None), P(both), P(both, None))
    return jax.shard_map(
        shards, mesh=mesh, in_specs=in_specs, out_specs=P(both, None), check_vma=False
    )
```

```python
import functools
import math

import jax
import jax.numpy as jnp
from jax import lax
from jax.experimental import pallas as pl
from jax.experimental.pallas import tpu as pltpu
from jax.sharding import PartitionSpec as P

HEAD_DIM = 128
BLOCK = 128
CHUNK_HEADS = 2
EARLY_CHUNKS = 4
POOL_HEADS = 8
MESH = pl.DeviceIdType.MESH


def dot_t(a, b):
    return lax.dot_general(a, b, (((1,), (1,)), ((), ())), preferred_element_type=jnp.float32)


def dot(a, b):
    return jnp.dot(a, b, preferred_element_type=jnp.float32)


def kernel(
    groups, seqs, pos_hbm, layout_hbm, q_hbm, k_hbm, v_hbm, out,
    pos_ref, layout_ref, q, k, v, halo, gathered, own, wide, bias,
    load_sem, send_sem, recv_sem, seq_send, seq_recv, grp_send, grp_recv,
):
    rows, width = q.shape
    heads = width // HEAD_DIM
    blocks = rows // BLOCK
    devices = groups * seqs
    total_blocks = devices * blocks
    step_cols = CHUNK_HEADS * HEAD_DIM
    chunks = heads // CHUNK_HEADS
    stages = groups.bit_length() - 1
    near = 2 * seqs

    g, s = lax.axis_index("grp"), lax.axis_index("seq")
    me = g * seqs + s
    has_left, has_right = me > 0, me < devices - 1
    left, right = lax.max(me - 1, 0), lax.min(me + 1, devices - 1)

    def coords(position):
        return (position // seqs, position % seqs)

    left_near = has_left & (me % near != 0)
    right_near = has_right & ((me + 1) % near != 0)
    left_far = has_left & (me % near == 0)
    right_far = has_right & ((me + 1) % near == 0)

    loads = [
        pltpu.make_async_copy(src, dst, load_sem.at[i])
        for i, (src, dst) in enumerate(((k_hbm, k), (v_hbm, v), (q_hbm, q), (pos_hbm, pos_ref), (layout_hbm, layout_ref)))
    ]
    barrier = pltpu.get_barrier_semaphore()

    def signal(device):
        pl.semaphore_signal(barrier, inc=1, device_id=device, device_id_type=MESH)

    @pl.when(has_left)
    def _():
        signal(coords(left))

    @pl.when(has_right)
    def _():
        signal(coords(right))

    for o in range(1, seqs):
        signal((g, lax.rem(s + o, seqs)))

    def partner(stage):
        size = 1 << stage
        bit = (g // size) % 2
        return g + size * (1 - 2 * bit)

    for stage in range(stages):
        signal((partner(stage), s))
    for load in loads:
        load.start()
    pl.semaphore_wait(
        barrier, seqs - 1 + stages + has_left.astype(jnp.int32) + has_right.astype(jnp.int32)
    )

    def edge(side, kv, c):
        src = (k, v)[kv]
        cols = pl.ds(pl.multiple_of(c * step_cols, step_cols), step_cols)
        first = rows - BLOCK if side == 0 else 0
        return pltpu.make_async_remote_copy(
            src_ref=src.at[pl.ds(first, BLOCK), cols],
            dst_ref=halo.at[side, kv, :, cols],
            send_sem=send_sem.at[side, kv, c],
            recv_sem=recv_sem.at[side, kv, c],
            device_id=coords(right if side == 0 else left),
            device_id_type=MESH,
        )

    def send_edges(side, when, lo, hi):
        @pl.when(when)
        def _():
            def body(c, carry):
                for kv in range(2):
                    edge(side, kv, c).start()
                return carry

            lax.fori_loop(lo, hi, body, 0)

    def send_both(when_right, when_left, lo, hi):
        both = when_right & when_left

        @pl.when(both)
        def _():
            def body(c, carry):
                for side in range(2):
                    for kv in range(2):
                        edge(side, kv, c).start()
                return carry

            lax.fori_loop(lo, hi, body, 0)

        send_edges(0, when_right & jnp.logical_not(when_left), lo, hi)
        send_edges(1, when_left & jnp.logical_not(when_right), lo, hi)

    loads[0].wait()
    loads[1].wait()
    early = min(EARLY_CHUNKS, chunks)
    later = (early + chunks) // 2
    send_both(right_near, left_near, 0, early)

    picks = (
        lax.broadcasted_iota(jnp.int32, (16, rows), 1) // BLOCK
        == lax.broadcasted_iota(jnp.int32, (16, rows), 0)
    ).astype(jnp.bfloat16)

    def pool(step, carry):
        for i in range(POOL_HEADS):
            h = step * POOL_HEADS + i
            cols = pl.ds(pl.multiple_of(h * HEAD_DIM, HEAD_DIM), HEAD_DIM)
            for kv, src in enumerate((k, v)):
                mean = dot(picks, src[:, cols])[:8] * (1.0 / BLOCK)
                spread = jnp.mean(mean * mean, axis=-1, keepdims=True)
                scaled = mean / jnp.sqrt(spread + 1e-06)
                for b in range(blocks):
                    own[pl.ds((kv * blocks + b) * heads + h, 1), :] = scaled[b : b + 1]
        return carry

    lax.fori_loop(0, heads // POOL_HEADS, pool, 0)
    gathered[me] = own[...].astype(jnp.bfloat16)

    def seq_copy(o):
        return pltpu.make_async_remote_copy(
            src_ref=gathered.at[pl.ds(me, 1)],
            dst_ref=gathered.at[pl.ds(me, 1)],
            send_sem=seq_send.at[o],
            recv_sem=seq_recv.at[o],
            device_id=(g, lax.rem(s + o, seqs)),
            device_id_type=MESH,
        )

    for o in range(1, seqs):
        seq_copy(o).start()

    send_both(right_near, left_near, early, chunks)

    loads[3].wait()
    loads[4].wait()
    ids = lax.broadcasted_iota(jnp.int32, (BLOCK, total_blocks), 1)
    spots = lax.broadcasted_iota(jnp.int32, (BLOCK, total_blocks), 0)
    for b in range(blocks):
        seen = spots == pos_ref[b]
        for link in range(layout_ref.shape[1]):
            seen = seen | (ids == layout_ref[b, link])
        bias[b * BLOCK : (b + 1) * BLOCK, :] = jnp.where(seen, 0.0, -jnp.inf)

    @pl.when(jnp.logical_not(has_left))
    def _():
        halo[0] = jnp.zeros(halo.shape[1:], halo.dtype)

    @pl.when(jnp.logical_not(has_right))
    def _():
        halo[1] = jnp.zeros(halo.shape[1:], halo.dtype)

    for o in range(1, seqs):
        seq_copy(o).wait()

    def grp_copy(stage):
        size = (1 << stage) * seqs
        first = (g // (1 << stage)) * size
        return pltpu.make_async_remote_copy(
            src_ref=gathered.at[pl.ds(first, size)],
            dst_ref=gathered.at[pl.ds(first, size)],
            send_sem=grp_send.at[stage],
            recv_sem=grp_recv.at[stage],
            device_id=(partner(stage), s),
            device_id_type=MESH,
        )

    for stage in range(stages):
        grp_copy(stage).start()
        if stage == stages - 2:
            send_both(right_far, left_far, 0, later)
        if stage == stages - 1:
            send_both(right_far, left_far, later if stages > 1 else early, chunks)
        grp_copy(stage).wait()

    def widen(d, carry):
        spread = blocks * heads
        at = pl.ds(pl.multiple_of(d * spread, spread), spread)
        for kv in range(2):
            wide[kv, at, :] = gathered[d, kv * spread : (kv + 1) * spread].astype(jnp.float32)
        return carry

    lax.fori_loop(0, devices, widen, 0)
    loads[2].wait()

    factor = math.log2(math.e) / math.sqrt(HEAD_DIM)
    left_bias = jnp.where(has_left, 0.0, -jnp.inf)
    right_bias = jnp.where(has_right, 0.0, -jnp.inf)

    def attend(c, carry):
        for side, there in ((0, has_left), (1, has_right)):
            @pl.when(there)
            def _(side=side):
                for kv in range(2):
                    edge(side, kv, c).wait_recv()

        for i in range(CHUNK_HEADS):
            h = c * CHUNK_HEADS + i
            cols = pl.ds(pl.multiple_of(h * HEAD_DIM, HEAD_DIM), HEAD_DIM)
            rows_of = pl.ds(h, total_blocks, stride=heads)
            qh, kh, vh = q[:, cols], k[:, cols], v[:, cols]
            sk = wide[0, rows_of, :].astype(jnp.bfloat16)
            sv = wide[1, rows_of, :].astype(jnp.bfloat16)
            kl, vl = halo[0, 0, :, cols], halo[0, 1, :, cols]
            kr, vr = halo[1, 0, :, cols], halo[1, 1, :, cols]
            s_own = dot_t(qh, kh)
            if blocks > 2:
                gap = (
                    lax.broadcasted_iota(jnp.int32, (rows, rows), 0) // BLOCK
                    - lax.broadcasted_iota(jnp.int32, (rows, rows), 1) // BLOCK
                )
                s_own = jnp.where(jnp.abs(gap) <= 1, s_own, -jnp.inf)
            s_left = dot_t(qh[:BLOCK], kl) + left_bias
            s_right = dot_t(qh[rows - BLOCK :], kr) + right_bias
            s_sum = dot_t(qh, sk) + bias[...]
            middle = [jnp.full((rows - 2 * BLOCK, BLOCK), -jnp.inf)] if blocks > 2 else []
            s_halo = jnp.concatenate([s_left, *middle, s_right], axis=0)
            peak = jnp.maximum(
                jnp.max(s_sum, axis=-1, keepdims=True),
                jnp.maximum(
                    jnp.max(s_own, axis=-1, keepdims=True),
                    jnp.max(s_halo, axis=-1, keepdims=True),
                ),
            )
            w_own = jnp.exp2((s_own - peak) * factor)
            w_halo = jnp.exp2((s_halo - peak) * factor)
            w_sum = jnp.exp2((s_sum - peak) * factor)
            total = (
                jnp.sum(w_own, axis=-1, keepdims=True)
                + jnp.sum(w_halo, axis=-1, keepdims=True)
                + jnp.sum(w_sum, axis=-1, keepdims=True)
            )
            r_halo = w_halo.astype(jnp.bfloat16)
            acc = dot(w_own.astype(jnp.bfloat16), vh) + dot(w_sum.astype(jnp.bfloat16), sv)
            middle = [jnp.zeros((rows - 2 * BLOCK, HEAD_DIM), jnp.float32)] if blocks > 2 else []
            acc = acc + jnp.concatenate(
                [dot(r_halo[:BLOCK], vl), *middle, dot(r_halo[rows - BLOCK :], vr)], axis=0
            )
            out[:, cols] = (acc / total).astype(jnp.bfloat16)
        return carry

    lax.fori_loop(0, chunks, attend, 0)

    def finish(c, carry):
        for side, there in ((0, has_right), (1, has_left)):
            @pl.when(there)
            def _(side=side):
                for kv in range(2):
                    edge(side, kv, c).wait_send()
        return carry

    lax.fori_loop(0, chunks, finish, 0)


def solution(mesh):
    groups, seqs = mesh.shape["grp"], mesh.shape["seq"]
    assert groups & (groups - 1) == 0

    def shards(queries, keys, values, global_pos, layout):
        rows, width = queries.shape
        blocks, heads = rows // BLOCK, width // HEAD_DIM
        devices = groups * seqs
        chunks = heads // CHUNK_HEADS
        stages = groups.bit_length() - 1
        summaries = devices * blocks * width
        limit = 2 * (4 * rows + 4 * BLOCK) * width + 12 * summaries + (8 << 20)
        operands = [
            pltpu.with_memory_space_constraint(a, pltpu.HBM)
            for a in (global_pos, layout, queries, keys, values)
        ]
        return pl.pallas_call(
            functools.partial(kernel, groups, seqs),
            out_shape=pltpu.VMEM((rows, width), jnp.bfloat16),
            in_specs=[pl.BlockSpec(memory_space=pltpu.HBM)] * 5,
            out_specs=pl.BlockSpec(memory_space=pltpu.VMEM),
            scratch_shapes=[
                pltpu.SMEM(global_pos.shape, jnp.int32),
                pltpu.SMEM(layout.shape, jnp.int32),
                pltpu.VMEM((rows, width), jnp.bfloat16),
                pltpu.VMEM((rows, width), jnp.bfloat16),
                pltpu.VMEM((rows, width), jnp.bfloat16),
                pltpu.VMEM((2, 2, BLOCK, width), jnp.bfloat16),
                pltpu.VMEM((devices, 2 * blocks * heads, HEAD_DIM), jnp.bfloat16),
                pltpu.VMEM((2 * blocks * heads, HEAD_DIM), jnp.float32),
                pltpu.VMEM((2, devices * blocks * heads, HEAD_DIM), jnp.float32),
                pltpu.VMEM((rows, devices * blocks), jnp.float32),
                pltpu.SemaphoreType.DMA((5,)),
                pltpu.SemaphoreType.DMA((2, 2, chunks)),
                pltpu.SemaphoreType.DMA((2, 2, chunks)),
                pltpu.SemaphoreType.DMA((seqs,)),
                pltpu.SemaphoreType.DMA((seqs,)),
                pltpu.SemaphoreType.DMA((max(stages, 1),)),
                pltpu.SemaphoreType.DMA((max(stages, 1),)),
            ],
            compiler_params=pltpu.CompilerParams(
                collective_id=0, has_side_effects=True, vmem_limit_bytes=limit
            ),
        )(*operands)

    both = ("grp", "seq")
    in_specs = (P(both, None), P(both, None), P(both, None), P(both), P(both, None))
    return jax.shard_map(
        shards, mesh=mesh, in_specs=in_specs, out_specs=P(both, None), check_vma=False
    )
```
